256 devices in a mesh: space: 64 (over z, y, core), tm: 4 (over x).
Axes of the slice: x: 4, y: 4, z: 8, core: 2. Of those that a mesh axis runs over, the one named last changes fastest.
Arguments:
- precip: float32 [512, 384, 2048], P('tm', 'space'), may hold values from 0.0001 to 0.01
Outputs:
- totals: float32 [384, 2048, 512], P(None, 'space', 'tm')
The draws below stay inside these ranges and needn't reach their ends.
All inputs are finite; a program needn't handle non-finite values.
Results may differ from the reference program's by a relative error of at most 0.00005.
Values sent between devices are 32-bit elements; how exact they have to be, the bound alone decides.
No kernel may reach another device: no remote copies, remote signals or barrier semaphores. Data moves between devices by JAX's collectives and lax.ppermute only.
A program may use at most 64 MiB of HBM per device.

```python
import math
import jax
import jax.numpy as jnp

LON = 2048
DAYS = 512
LAT = 384


def steps_of(rng, dims, split, least, high):
    def one(position, blocks):
        steps = jax.random.uniform(jax.random.fold_in(jax.random.fold_in(rng, 6), position), (blocks,), jnp.float32, least / len(split), high / len(split))
        return jnp.repeat(jnp.exp(steps), dims[position] // blocks).reshape((-1,) + (1,) * (len(dims) - position - 1))

    factor_of = one(*split[0])
    for cut in split[1:]:
        factor_of = factor_of * one(*cut)
    return factor_of


def setup_inputs(seed: int = 0) -> dict:
    key_list = jax.random.split(jax.random.key(seed), 2)
    precip = jnp.clip(jnp.exp(math.log(0.01) - 4.6051702 * jax.random.uniform(key_list[0], (DAYS, LAT, LON), jnp.float32) ** steps_of(key_list[0], (DAYS, LAT, LON), ((0, 4), (1, 64)), -0.2, 0.2)), 0.0001, 0.01)
    return {"precip": precip}


def reference(precip):
    running = jnp.cumsum(precip, axis=0)
    return jnp.transpose(running, (1, 2, 0))
```

```python
import functools

import jax
import jax.numpy as jnp
from jax import lax
from jax.experimental import pallas as pl
from jax.experimental.pallas import tpu as pltpu
from jax.sharding import Mesh
from jax.sharding import PartitionSpec as P

PLANE = ("space_1", "space_2")
EARLY = (3, -3)
NEAR = (1, -1)
PLANE_FIRST = (0, 4, 2, -2)

IN_VMEM = pl.BlockSpec(memory_space=pltpu.VMEM)
IN_HBM = pl.BlockSpec(memory_space=pl.ANY)
IN_SMEM = pl.BlockSpec(memory_space=pltpu.SMEM)
TOKEN = (8, 128)
LIMIT = pltpu.CompilerParams(vmem_limit_bytes=12 * 2**20)


def vmem(shape):
    return pltpu.VMEM(shape, jnp.float32)


def hbm(shape):
    return pltpu.HBM(shape, jnp.float32)


def ring_place(where_ref, step, ring):
    return lax.rem(where_ref[0] + (step + ring), ring)


def carried(theirs_ref, blocks_before, row, lanes):
    carry = None
    for q in range(theirs_ref.shape[0]):
        line = jnp.where(q < blocks_before, theirs_ref[q, pl.ds(row, 1), lanes], 0.0)
        carry = line if carry is None else carry + line
    return carry


def running_kernel(where_ref, days_ref, theirs_ref, *refs, steps, ring, stacked):
    n = len(steps)
    *out_refs, done_ref, days_buf, out_buf, in_sems, out_sems = refs
    rows, days, lon = days_ref.shape
    width = lon // ring
    plane, cell = out_buf.shape[1], out_buf.shape[3]
    lanes = [
        pl.ds(pl.multiple_of(ring_place(where_ref, s, ring) * width, width), width) for s in steps
    ]
    reads = [
        [
            pltpu.make_async_copy(days_ref.at[r, :, lanes[k]], days_buf.at[k, r], in_sems.at[k, r])
            for r in range(rows)
        ]
        for k in range(n)
    ]
    writes = [
        pltpu.make_async_copy(
            out_buf.at[k], out_refs[0].at[:, k] if stacked else out_refs[k], out_sems.at[k]
        )
        for k in range(n)
    ]
    for line in reads:
        for copy in line:
            copy.start()
    earlier = lax.broadcasted_iota(jnp.int32, (days, days), 0)
    later = lax.broadcasted_iota(jnp.int32, (days, days), 1)
    upto = (earlier <= later).astype(jnp.bfloat16)
    first = lax.broadcasted_iota(jnp.int32, (days, width), 0) == 0
    dot = functools.partial(jnp.dot, preferred_element_type=jnp.float32)
    for k in range(n):
        for r in range(rows):
            reads[k][r].wait()
            x = days_buf[k, r]
            if theirs_ref is not None:
                x = jnp.where(first, x + carried(theirs_ref, where_ref[1], r, lanes[k]), x)
            x = x.T
            high = x.astype(jnp.bfloat16)
            rest = x - high.astype(jnp.float32)
            mid = rest.astype(jnp.bfloat16)
            low = (rest - mid.astype(jnp.float32)).astype(jnp.bfloat16)
            total = dot(high, upto) + (dot(mid, upto) + dot(low, upto))
            out_buf[k, :, r] = total.reshape(plane, cell, days)
        writes[k].start()
    done_ref[...] = jnp.zeros_like(done_ref)
    for copy in writes:
        copy.wait()


def running(where, by_row, theirs, token, ring, steps, stacked, plane):
    rows, days, lon = by_row.shape
    width = lon // ring
    cell = width // plane
    n = len(steps)
    outs = [hbm((plane, n, rows, cell, days))] if stacked else [hbm((plane, rows, cell, days))] * n
    args = [where, by_row]
    specs = [IN_SMEM, IN_HBM]
    for extra in (theirs, token):
        if extra is not None:
            args.append(extra)
            specs.append(IN_VMEM)

    def body(where_ref, days_ref, *refs):
        refs = list(refs)
        theirs_ref = None if theirs is None else refs.pop(0)
        if token is not None:
            refs.pop(0)
        running_kernel(where_ref, days_ref, theirs_ref, *refs, steps=steps, ring=ring, stacked=stacked)

    *made, done = pl.pallas_call(
        body,
        compiler_params=LIMIT,
        in_specs=specs,
        out_specs=[IN_HBM] * len(outs) + [IN_VMEM],
        out_shape=[*outs, jax.ShapeDtypeStruct(TOKEN, jnp.float32)],
        scratch_shapes=[
            pltpu.VMEM((n, rows, days, width), jnp.float32),
            pltpu.VMEM((n, plane, rows, cell, days), jnp.float32),
            pltpu.SemaphoreType.DMA((n, rows)),
            pltpu.SemaphoreType.DMA((n,)),
        ],
    )(*args)
    return made, done


def totals_kernel(days_ref, token_ref, total_ref, days_buf, sems):
    rows, _, lon = days_ref.shape
    cuts = sems.shape[0]
    width = lon // cuts
    copies = [
        pltpu.make_async_copy(
            days_ref.at[:, :, pl.ds(c * width, width)], days_buf.at[:, :, pl.ds(c * width, width)], sems.at[c]
        )
        for c in range(cuts)
    ]
    for copy in copies:
        copy.start()
    for c in range(cuts):
        copies[c].wait()
        for r in range(rows):
            line = jnp.sum(days_buf[r, :, pl.ds(c * width, width)], axis=0, keepdims=True)
            for q in range(total_ref.shape[0]):
                total_ref[q, pl.ds(r, 1), pl.ds(c * width, width)] = line


def block_totals(by_row, token, copies, cuts=8):
    rows, _, lon = by_row.shape
    return pl.pallas_call(
        totals_kernel,
        compiler_params=LIMIT,
        in_specs=[IN_HBM, IN_VMEM],
        out_specs=IN_VMEM,
        out_shape=vmem((copies, rows, lon)),
        scratch_shapes=[pltpu.VMEM(by_row.shape, jnp.float32), pltpu.SemaphoreType.DMA((cuts,))],
    )(by_row, (token))


def lines_kernel(where_ref, theirs_ref, token_ref, *refs, steps, ring):
    *line_refs, done_ref = refs
    width = theirs_ref.shape[2] // ring
    for step, line_ref in zip(steps, line_refs):
        lanes = pl.ds(pl.multiple_of(ring_place(where_ref, step, ring) * width, width), width)
        line_ref[...] = jnp.zeros_like(line_ref)
        for r in range(theirs_ref.shape[1]):
            line_ref[pl.ds(r, 1)] = carried(theirs_ref, where_ref[1], r, lanes)
    done_ref[...] = jnp.zeros_like(done_ref)


def carry_lines(where, theirs, token, steps, ring):
    width = theirs.shape[2] // ring
    *lines, done = pl.pallas_call(
        functools.partial(lines_kernel, steps=steps, ring=ring),
        compiler_params=LIMIT,
        in_specs=[IN_SMEM, IN_VMEM, IN_VMEM],
        out_specs=[IN_VMEM] * (len(steps) + 1),
        out_shape=[vmem((8, width))] * len(steps) + [vmem(TOKEN)],
    )(where, (theirs), (token))
    return lines, done


def gather_kernel(*refs):
    *refs, out_ref = refs
    plane, n, _, cell, days = out_ref.shape
    block_refs, line_refs = refs[:n], refs[n:-1]
    row = pl.program_id(0)
    for k in range(n):
        block = block_refs[k][:, 0]
        if k < len(line_refs):
            carry = jnp.broadcast_to(line_refs[k][pl.ds(row, 1)], (days, plane * cell)).T
            block = block + carry.reshape(plane, cell, days)
        out_ref[:, k, 0] = block


def gathered(blocks, lines, token):
    plane, rows, cell, days = blocks[0].shape
    n = len(blocks)
    return pl.pallas_call(
        gather_kernel,
        compiler_params=LIMIT,
        grid=(rows,),
        in_specs=[pl.BlockSpec((plane, 1, cell, days), lambda r: (0, r, 0, 0))] * n
        + [pl.BlockSpec(line.shape, lambda r: (0, 0)) for line in lines]
        + [pl.BlockSpec(memory_space=pl.ANY)],
        out_specs=pl.BlockSpec((plane, n, 1, cell, days), lambda r: (0, 0, r, 0, 0)),
        out_shape=jax.ShapeDtypeStruct((plane, n, rows, cell, days), jnp.float32),
    )(*blocks, *lines, token)


def place_kernel(where_ref, piece_ref, *refs):
    refs[-1][...] = piece_ref[...].reshape(refs[-1].shape)


def place(where, whole, ring, piece, steps):
    plane, _, rows, cell, days = piece.shape
    half = plane // 2

    def target(j, h, where):
        step = jnp.int32(steps[0])
        for i, s in enumerate(steps[1:], 1):
            step = jnp.where(j == i, s, step)
        return (lax.rem(where[0] - step + 2 * ring, ring), h, 0, 0, 0)

    args = (where, piece) if whole is None else (where, piece, whole)
    in_specs = [pl.BlockSpec((half, 1, rows, cell, days), lambda j, h, where: (h, j, 0, 0, 0))]
    if whole is not None:
        in_specs.append(pl.BlockSpec(memory_space=pl.ANY))
    return pl.pallas_call(
        place_kernel,
        compiler_params=LIMIT,
        grid_spec=pltpu.PrefetchScalarGridSpec(
            num_scalar_prefetch=1,
            grid=(len(steps), 2),
            in_specs=in_specs,
            out_specs=pl.BlockSpec((1, half, rows, cell, days), target),
        ),
        out_shape=jax.ShapeDtypeStruct((ring, plane, rows, cell, days), jnp.float32),
        input_output_aliases={} if whole is None else {2: 0},
    )(*args)


def place_block(where, whole, block, step):
    ring = whole.shape[0]
    at = lax.rem(where[0] - step + ring, ring)
    return lax.dynamic_update_slice(whole, block[None], (at, 0, 0, 0, 0))


def shifted(block, ring, step):
    return lax.ppermute(block, "space_0", [(i, (i + step) % ring) for i in range(ring)])


def exchanged(value, axes):
    return lax.all_to_all(value, axes, split_axis=0, concat_axis=0, tiled=True)


def per_device(precip):
    by_row = jnp.transpose(precip, (1, 0, 2))
    by_row = pltpu.with_memory_space_constraint(by_row, pltpu.HBM)
    rows, days, lon = by_row.shape
    ring = lax.axis_size("space_0")
    plane = lax.axis_size("space_1") * lax.axis_size("space_2")
    blocks = lax.axis_size("tm")
    where = jnp.stack([lax.axis_index("space_0"), lax.axis_index("tm")]).astype(jnp.int32)

    def sent(block, step):
        return shifted(block, ring, step)

    early, token = running(where, by_row, None, None, ring, EARLY, False, plane)
    early = [sent(block, step) for block, step in zip(early, EARLY)]
    theirs = block_totals(by_row, token, blocks)
    theirs = exchanged(theirs, "tm")
    (first,), token = running(where, by_row, theirs, None, ring, PLANE_FIRST, True, plane)
    mixed = exchanged(first, PLANE)
    near, token = running(where, by_row, theirs, token, ring, NEAR, False, plane)
    near = [sent(block, step) for block, step in zip(near, NEAR)]
    lines, token = carry_lines(where, theirs, token, EARLY, ring)
    lines = [sent(line, step) for line, step in zip(lines, EARLY)]
    late = [sent(mixed[:, k], PLANE_FIRST[k]) for k in (1, 2, 3)]
    second = gathered([*early, *near], lines, token)
    second = exchanged(second, PLANE)
    whole = place(where, None, ring, mixed, (0,))
    whole = place(where, whole, ring, second, (*EARLY, *NEAR))
    for k in (3, 2, 1):
        whole = place_block(where, whole, late[k - 1], PLANE_FIRST[k])
    return whole.reshape(ring * plane * rows, lon // (ring * plane), days)


def solution(mesh):
    finer = Mesh(
        mesh.devices.reshape(8, 4, 2, mesh.shape["tm"]), ("space_0", "space_1", "space_2", "tm")
    )
    space = ("space_0", "space_1", "space_2")
    return jax.shard_map(
        per_device,
        mesh=finer,
        in_specs=(P("tm", space, None),),
        out_specs=P(None, space, "tm"),
        check_vma=False,
    )
```

```python
import functools

import jax
import jax.numpy as jnp
from jax import lax
from jax.experimental import pallas as pl
from jax.experimental.pallas import tpu as pltpu
from jax.sharding import Mesh
from jax.sharding import PartitionSpec as P

PLANE = ("space_1", "space_2")
RING_FIRST = (4, 3, -3)
PLANE_FIRST = (0, 2, -2, 1, -1)
PARTS = 3

IN_VMEM = pl.BlockSpec(memory_space=pltpu.VMEM)
IN_HBM = pl.BlockSpec(memory_space=pl.ANY)
IN_SMEM = pl.BlockSpec(memory_space=pltpu.SMEM)
LIMIT = pltpu.CompilerParams(vmem_limit_bytes=12 * 2**20)


def hbm(shape):
    return pltpu.HBM(shape, jnp.float32)


def ring_place(where_ref, step, ring):
    return lax.rem(where_ref[0] + (step + ring), ring)


def carried(theirs_ref, blocks_before, row, lanes):
    carry = None
    for q in range(theirs_ref.shape[0]):
        line = jnp.where(q < blocks_before, theirs_ref[q, pl.ds(row, 1), lanes], 0.0)
        carry = line if carry is None else carry + line
    return carry


def running_kernel(sources, carry_of, out_ref, days_buf, parts_buf, out_buf, in_sems, out_sems):
    n = len(sources)
    rows, days, width = days_buf.shape[1:]
    plane, cell = out_buf.shape[1], out_buf.shape[3]
    reads = [pltpu.make_async_copy(sources[k], days_buf.at[k], in_sems.at[k]) for k in range(n)]
    writes = [
        pltpu.make_async_copy(out_buf.at[k], out_ref.at[:, k], out_sems.at[k]) for k in range(n)
    ]
    for copy in reads:
        copy.start()
    earlier = lax.broadcasted_iota(jnp.int32, (days, days), 0)
    later = lax.broadcasted_iota(jnp.int32, (days, days), 1)
    upto = (earlier <= later).astype(jnp.bfloat16)
    upto = jnp.concatenate([upto] * PARTS, 0)
    first = lax.broadcasted_iota(jnp.int32, (days, width), 0) == 0
    for k in range(n):
        reads[k].wait()
        for r in range(rows):
            x = days_buf[k, r]
            x = jnp.where(first, x + carry_of(k, r), x).T
            for p in range(PARTS):
                part = x.astype(jnp.bfloat16)
                parts_buf[k % 2, r, :, pl.ds(p * days, days)] = part
                x = x - part.astype(jnp.float32)
        for r in range(rows):
            total = jnp.dot(parts_buf[k % 2, r], upto, preferred_element_type=jnp.float32)
            out_buf[k, :, r] = total.reshape(plane, cell, days)
        writes[k].start()
    for copy in writes:
        copy.wait()


def column_kernel(where_ref, days_ref, theirs_ref, out_ref, *scratch, steps, ring):
    width = days_ref.shape[2] // ring
    lanes = [
        pl.ds(pl.multiple_of(ring_place(where_ref, s, ring) * width, width), width) for s in steps
    ]
    running_kernel(
        [days_ref.at[:, :, part] for part in lanes],
        lambda k, r: carried(theirs_ref, where_ref[1], r, lanes[k]),
        out_ref,
        *scratch,
    )


def cut_kernel(where_ref, days_ref, *refs, steps, ring):
    n = len(steps)
    out_refs, buf, in_sems, out_sems = refs[:n], refs[n], refs[n + 1], refs[n + 2]
    width = days_ref.shape[2] // ring
    reads, writes = [], []
    for k, step in enumerate(steps):
        lanes = pl.ds(pl.multiple_of(ring_place(where_ref, step, ring) * width, width), width)
        reads.append(pltpu.make_async_copy(days_ref.at[:, :, lanes], buf.at[k], in_sems.at[k]))
        writes.append(pltpu.make_async_copy(buf.at[k], out_refs[k], out_sems.at[k]))
    for copy in reads:
        copy.start()
    for read, write in zip(reads, writes):
        read.wait()
        write.start()
    for copy in writes:
        copy.wait()


def cut_columns(where, by_row, ring, steps):
    rows, days, lon = by_row.shape
    n = len(steps)
    shape = (rows, days, lon // ring)
    return pl.pallas_call(
        functools.partial(cut_kernel, steps=steps, ring=ring),
        compiler_params=LIMIT,
        in_specs=[IN_SMEM, IN_HBM],
        out_specs=[IN_HBM] * n,
        out_shape=[hbm(shape)] * n,
        scratch_shapes=[
            pltpu.VMEM((n, *shape), jnp.float32),
            pltpu.SemaphoreType.DMA((n,)),
            pltpu.SemaphoreType.DMA((n,)),
        ],
    )(where, by_row)


def block_kernel(*refs, n):
    blocks, lines, rest = refs[:n], refs[n : 2 * n], refs[2 * n :]
    out_ref, *scratch = rest[-6:]
    running_kernel(blocks, lambda k, r: lines[k][pl.ds(r, 1)], out_ref, *scratch)


def running_call(body, specs, args, n, rows, days, width, plane):
    cell = width // plane
    return pl.pallas_call(
        body,
        compiler_params=LIMIT,
        in_specs=specs,
        out_specs=IN_HBM,
        out_shape=hbm((plane, n, rows, cell, days)),
        scratch_shapes=[
            pltpu.VMEM((n, rows, days, width), jnp.float32),
            pltpu.VMEM((2, rows, width, PARTS * days), jnp.bfloat16),
            pltpu.VMEM((n, plane, rows, cell, days), jnp.float32),
            pltpu.SemaphoreType.DMA((n,)),
            pltpu.SemaphoreType.DMA((n,)),
        ],
    )(*args)


def running_columns(where, by_row, theirs, ring, steps, plane):
    rows, days, lon = by_row.shape
    body = functools.partial(column_kernel, steps=steps, ring=ring)
    specs = [IN_SMEM, IN_HBM, IN_VMEM]
    args = (where, by_row, theirs)
    return running_call(body, specs, args, len(steps), rows, days, lon // ring, plane)


def running_blocks(blocks, lines, plane):
    n = len(blocks)
    body = functools.partial(block_kernel, n=n)
    specs = [IN_HBM] * n + [IN_VMEM] * n
    return running_call(body, specs, (*blocks, *lines), n, *blocks[0].shape, plane)


def totals_kernel(days_ref, total_ref, days_buf, sems):
    rows, _, lon = days_ref.shape
    cuts = sems.shape[0]
    width = lon // cuts
    copies = [
        pltpu.make_async_copy(
            days_ref.at[:, :, pl.ds(c * width, width)], days_buf.at[:, :, pl.ds(c * width, width)], sems.at[c]
        )
        for c in range(cuts)
    ]
    for copy in copies:
        copy.start()
    for c in range(cuts):
        copies[c].wait()
        for r in range(rows):
            line = jnp.sum(days_buf[r, :, pl.ds(c * width, width)], axis=0, keepdims=True)
            for q in range(total_ref.shape[0]):
                total_ref[q, pl.ds(r, 1), pl.ds(c * width, width)] = line


def block_totals(by_row, copies, cuts=8):
    rows, _, lon = by_row.shape
    return pl.pallas_call(
        totals_kernel,
        compiler_params=LIMIT,
        in_specs=[IN_HBM],
        out_specs=IN_VMEM,
        out_shape=jax.ShapeDtypeStruct((copies, rows, lon), jnp.float32),
        scratch_shapes=[pltpu.VMEM(by_row.shape, jnp.float32), pltpu.SemaphoreType.DMA((cuts,))],
    )(by_row)


def lines_kernel(where_ref, theirs_ref, *line_refs, steps, ring):
    width = theirs_ref.shape[2] // ring
    for step, line_ref in zip(steps, line_refs):
        lanes = pl.ds(pl.multiple_of(ring_place(where_ref, step, ring) * width, width), width)
        line_ref[...] = jnp.zeros_like(line_ref)
        for r in range(theirs_ref.shape[1]):
            line_ref[pl.ds(r, 1)] = carried(theirs_ref, where_ref[1], r, lanes)


def carry_lines(where, theirs, steps, ring):
    width = theirs.shape[2] // ring
    return pl.pallas_call(
        functools.partial(lines_kernel, steps=steps, ring=ring),
        compiler_params=LIMIT,
        in_specs=[IN_SMEM, IN_VMEM],
        out_specs=[IN_VMEM] * len(steps),
        out_shape=[jax.ShapeDtypeStruct((8, width), jnp.float32)] * len(steps),
    )(where, theirs)


def place_kernel(where_ref, piece_ref, *refs):
    refs[-1][...] = piece_ref[...].reshape(refs[-1].shape)


def place(where, whole, ring, piece, steps):
    plane, _, rows, cell, days = piece.shape
    half = plane // 2

    def target(j, h, where):
        step = jnp.int32(steps[0])
        for i, s in enumerate(steps[1:], 1):
            step = jnp.where(j == i, s, step)
        return (lax.rem(where[0] - step + 2 * ring, ring), h, 0, 0, 0)

    args = (where, piece) if whole is None else (where, piece, whole)
    in_specs = [pl.BlockSpec((half, 1, rows, cell, days), lambda j, h, where: (h, j, 0, 0, 0))]
    if whole is not None:
        in_specs.append(pl.BlockSpec(memory_space=pl.ANY))
    return pl.pallas_call(
        place_kernel,
        compiler_params=LIMIT,
        grid_spec=pltpu.PrefetchScalarGridSpec(
            num_scalar_prefetch=1,
            grid=(len(steps), 2),
            in_specs=in_specs,
            out_specs=pl.BlockSpec((1, half, rows, cell, days), target),
        ),
        out_shape=jax.ShapeDtypeStruct((ring, plane, rows, cell, days), jnp.float32),
        input_output_aliases={} if whole is None else {2: 0},
    )(*args)


def place_pair_kernel(where_ref, *refs, steps):
    n = len(steps)
    block_refs, whole_ref, sems = refs[:n], refs[n + 1], refs[n + 2]
    ring = whole_ref.shape[0]
    copies = [
        pltpu.make_async_copy(
            block_refs[k], whole_ref.at[ring_place(where_ref, -step, ring)], sems.at[k]
        )
        for k, step in enumerate(steps)
    ]
    for copy in copies:
        copy.start()
    for copy in copies:
        copy.wait()


def place_blocks(where, whole, blocks, steps):
    n = len(steps)
    blocks = [pltpu.with_memory_space_constraint(block, pltpu.VMEM) for block in blocks]
    return pl.pallas_call(
        functools.partial(place_pair_kernel, steps=steps),
        compiler_params=LIMIT,
        in_specs=[IN_SMEM] + [IN_VMEM] * n + [IN_HBM],
        out_specs=IN_HBM,
        out_shape=jax.ShapeDtypeStruct(whole.shape, jnp.float32),
        scratch_shapes=[pltpu.SemaphoreType.DMA((n,))],
        input_output_aliases={n + 1: 0},
    )(where, *blocks, whole)


def shifted(block, ring, step):
    return lax.ppermute(block, "space_0", [(i, (i + step) % ring) for i in range(ring)])


def exchanged(value, axes):
    return lax.all_to_all(value, axes, split_axis=0, concat_axis=0, tiled=True)


def per_device(precip):
    by_row = jnp.transpose(precip, (1, 0, 2))
    stays = pltpu.with_memory_space_constraint(by_row, pltpu.HBM)
    rows, days, lon = by_row.shape
    ring = lax.axis_size("space_0")
    plane = lax.axis_size("space_1") * lax.axis_size("space_2")
    blocks = lax.axis_size("tm")
    where = jnp.stack([lax.axis_index("space_0"), lax.axis_index("tm")]).astype(jnp.int32)

    def sent(block, step):
        return shifted(block, ring, step)

    def column(step):
        at = lax.rem(where[0] + (step + ring), ring) * (lon // ring)
        return lax.dynamic_slice(by_row, (0, 0, at), (rows, days, lon // ring))

    raw = [sent(column(RING_FIRST[0]), RING_FIRST[0])]
    cut = cut_columns(where, stays, ring, RING_FIRST[1:])
    raw += [sent(cut[k - 1], RING_FIRST[k]) for k in (1, 2)]
    theirs = block_totals(stays, blocks)
    theirs = exchanged(theirs, "tm")
    mixed = running_columns(where, stays, theirs, ring, PLANE_FIRST, plane)
    mixed = exchanged(mixed, PLANE)
    lines = carry_lines(where, theirs, RING_FIRST, ring)
    lines = [sent(line, step) for line, step in zip(lines, RING_FIRST)]
    late = [sent(mixed[:, k], PLANE_FIRST[k]) for k in range(1, len(PLANE_FIRST))]
    second = running_blocks(raw, lines, plane)
    second = exchanged(second, PLANE)
    whole = place(where, None, ring, mixed, (0,))
    whole = place(where, whole, ring, second, RING_FIRST)
    whole = place_blocks(where, whole, late[2:], PLANE_FIRST[3:])
    whole = place_blocks(where, whole, late[:2], PLANE_FIRST[1:3])
    return whole.reshape(ring * plane * rows, lon // (ring * plane), days)


def solution(mesh):
    finer = Mesh(
        mesh.devices.reshape(8, 4, 2, mesh.shape["tm"]), ("space_0", "space_1", "space_2", "tm")
    )
    space = ("space_0", "space_1", "space_2")
    return jax.shard_map(
        per_device,
        mesh=finer,
        in_specs=(P("tm", space, None),),
        out_specs=P(None, space, "tm"),
        check_vma=False,
    )
```

```python
import functools

import jax
import jax.numpy as jnp
from jax import lax
from jax.experimental import pallas as pl
from jax.experimental.pallas import tpu as pltpu
from jax.sharding import Mesh
from jax.sharding import PartitionSpec as P

PLANE = ("space_1", "space_2")
RING_FIRST = (4, 3, -3)
PLANE_FIRST = (0, 1, -1, 2, -2)
PARTS = 3
PIECES = 4

IN_VMEM = pl.BlockSpec(memory_space=pltpu.VMEM)
IN_HBM = pl.BlockSpec(memory_space=pl.ANY)
LIMIT = pltpu.CompilerParams(vmem_limit_bytes=12 * 2**20)
JOIN = pltpu.CompilerParams(vmem_limit_bytes=65_300_000)
WIDE = pltpu.CompilerParams(vmem_limit_bytes=64_800_000)


def hbm(shape):
    return pltpu.HBM(shape, jnp.float32)


def ring_place(step, ring):
    return lax.rem(lax.axis_index("space_0") + (step + ring), ring)


def carried(theirs_ref, blocks_before, row, lanes):
    carry = None
    for q in range(theirs_ref.shape[0]):
        line = jnp.where(q < blocks_before, theirs_ref[q, pl.ds(row, 1), lanes], 0.0)
        carry = line if carry is None else carry + line
    return carry


def running_kernel(sources, carry_of, out_ref, days_buf, parts_buf, out_buf, in_sems, out_sems):
    n = len(sources)
    rows, days, width = days_buf.shape[1:]
    plane, cell = out_buf.shape[1], out_buf.shape[3]
    reads = [pltpu.make_async_copy(sources[k], days_buf.at[k], in_sems.at[k]) for k in range(n)]
    writes = [
        pltpu.make_async_copy(out_buf.at[k], out_ref.at[:, k], out_sems.at[k]) for k in range(n)
    ]
    for copy in reads:
        copy.start()
    earlier = lax.broadcasted_iota(jnp.int32, (days, days), 0)
    later = lax.broadcasted_iota(jnp.int32, (days, days), 1)
    upto = (earlier <= later).astype(jnp.bfloat16)
    upto = jnp.concatenate([upto] * PARTS, 0)
    first = lax.broadcasted_iota(jnp.int32, (days, width), 0) == 0
    for k in range(n):
        reads[k].wait()
        for r in range(rows):
            x = days_buf[k, r]
            x = jnp.where(first, x + carry_of(k, r), x).T
            for p in range(PARTS):
                part = x.astype(jnp.bfloat16)
                parts_buf[k % 2, r, :, pl.ds(p * days, days)] = part
                x = x - part.astype(jnp.float32)
        for r in range(rows):
            total = jnp.dot(parts_buf[k % 2, r], upto, preferred_element_type=jnp.float32)
            out_buf[k, :, r] = total.reshape(plane, cell, days)
        writes[k].start()
    for copy in writes:
        copy.wait()


def column_kernel(days_ref, theirs_ref, out_ref, *scratch, steps, ring):
    width = days_ref.shape[2] // ring
    lanes = [
        pl.ds(pl.multiple_of(ring_place(s, ring) * width, width), width) for s in steps
    ]
    running_kernel(
        [days_ref.at[:, :, part] for part in lanes],
        lambda k, r: carried(theirs_ref, lax.axis_index("tm"), r, lanes[k]),
        out_ref,
        *scratch,
    )


def cut_kernel(days_ref, *refs, steps, ring):
    n = len(steps)
    out_refs, buf, in_sems, out_sems = refs[:n], refs[n], refs[n + 1], refs[n + 2]
    width = days_ref.shape[2] // ring
    reads, writes = [], []
    for k, step in enumerate(steps):
        lanes = pl.ds(pl.multiple_of(ring_place(step, ring) * width, width), width)
        reads.append(pltpu.make_async_copy(days_ref.at[:, :, lanes], buf.at[k], in_sems.at[k]))
        writes.append(pltpu.make_async_copy(buf.at[k], out_refs[k], out_sems.at[k]))
    for copy in reads:
        copy.start()
    for read, write in zip(reads, writes):
        read.wait()
        write.start()
    for copy in writes:
        copy.wait()


def cut_columns(by_row, ring, steps):
    rows, days, lon = by_row.shape
    n = len(steps)
    shape = (rows, days, lon // ring)
    return pl.pallas_call(
        functools.partial(cut_kernel, steps=steps, ring=ring),
        compiler_params=LIMIT,
        in_specs=[IN_HBM],
        out_specs=[IN_HBM] * n,
        out_shape=[hbm(shape)] * n,
        scratch_shapes=[
            pltpu.VMEM((n, *shape), jnp.float32),
            pltpu.SemaphoreType.DMA((n,)),
            pltpu.SemaphoreType.DMA((n,)),
        ],
    )(by_row)


def lead_kernel(days_ref, out_ref, sem, *, step, ring):
    width = days_ref.shape[2] // ring
    lanes = pl.ds(pl.multiple_of(ring_place(step, ring) * width, width), width)
    copy = pltpu.make_async_copy(days_ref.at[:, :, lanes], out_ref, sem)
    copy.start()
    copy.wait()


def lead_column(by_row, ring, step):
    rows, days, lon = by_row.shape
    return pl.pallas_call(
        functools.partial(lead_kernel, step=step, ring=ring),
        compiler_params=LIMIT,
        in_specs=[IN_HBM],
        out_specs=IN_VMEM,
        out_shape=pltpu.VMEM((rows, days, lon // ring), jnp.float32),
        scratch_shapes=[pltpu.SemaphoreType.DMA],
    )(by_row)


def block_kernel(*refs, n):
    blocks, lines, rest = refs[:n], refs[n : 2 * n], refs[2 * n :]
    out_ref, *scratch = rest[-6:]
    running_kernel(blocks, lambda k, r: lines[k][pl.ds(r, 1)], out_ref, *scratch)


def running_call(body, specs, args, n, rows, days, width, plane, params=LIMIT):
    cell = width // plane
    return pl.pallas_call(
        body,
        compiler_params=params,
        in_specs=specs,
        out_specs=IN_HBM,
        out_shape=hbm((plane, n, rows, cell, days)),
        scratch_shapes=[
            pltpu.VMEM((n, rows, days, width), jnp.float32),
            pltpu.VMEM((2, rows, width, PARTS * days), jnp.bfloat16),
            pltpu.VMEM((n, plane, rows, cell, days), jnp.float32),
            pltpu.SemaphoreType.DMA((n,)),
            pltpu.SemaphoreType.DMA((n,)),
        ],
    )(*args)


def running_columns(by_row, theirs, ring, steps, plane):
    rows, days, lon = by_row.shape
    body = functools.partial(column_kernel, steps=steps, ring=ring)
    specs = [IN_HBM, IN_VMEM]
    args = (by_row, theirs)
    return running_call(body, specs, args, len(steps), rows, days, lon // ring, plane)


def running_blocks(blocks, lines, plane):
    n = len(blocks)
    body = functools.partial(block_kernel, n=n)
    specs = [IN_HBM] * n + [IN_VMEM] * n
    return running_call(body, specs, (*blocks, *lines), n, *blocks[0].shape, plane, JOIN)


def totals_kernel(days_ref, total_ref, days_buf, sems):
    rows, _, lon = days_ref.shape
    cuts = sems.shape[0]
    width = lon // cuts
    copies = [
        pltpu.make_async_copy(
            days_ref.at[:, :, pl.ds(c * width, width)], days_buf.at[:, :, pl.ds(c * width, width)], sems.at[c]
        )
        for c in range(cuts)
    ]
    for copy in copies:
        copy.start()
    for c in range(cuts):
        copies[c].wait()
        for r in range(rows):
            line = jnp.sum(days_buf[r, :, pl.ds(c * width, width)], axis=0, keepdims=True)
            for q in range(total_ref.shape[0]):
                total_ref[q, pl.ds(r, 1), pl.ds(c * width, width)] = line


def block_totals(by_row, copies, cuts=8):
    rows, _, lon = by_row.shape
    return pl.pallas_call(
        totals_kernel,
        compiler_params=LIMIT,
        in_specs=[IN_HBM],
        out_specs=IN_VMEM,
        out_shape=jax.ShapeDtypeStruct((copies, rows, lon), jnp.float32),
        scratch_shapes=[pltpu.VMEM(by_row.shape, jnp.float32), pltpu.SemaphoreType.DMA((cuts,))],
    )(by_row)


def lines_kernel(theirs_ref, *line_refs, steps, ring):
    width = theirs_ref.shape[2] // ring
    for step, line_ref in zip(steps, line_refs):
        lanes = pl.ds(pl.multiple_of(ring_place(step, ring) * width, width), width)
        line_ref[...] = jnp.zeros_like(line_ref)
        for r in range(theirs_ref.shape[1]):
            line_ref[pl.ds(r, 1)] = carried(theirs_ref, lax.axis_index("tm"), r, lanes)


def carry_lines(theirs, steps, ring):
    width = theirs.shape[2] // ring
    return pl.pallas_call(
        functools.partial(lines_kernel, steps=steps, ring=ring),
        compiler_params=LIMIT,
        in_specs=[IN_VMEM],
        out_specs=[IN_VMEM] * len(steps),
        out_shape=[jax.ShapeDtypeStruct((8, width), jnp.float32)] * len(steps),
    )(theirs)


def place_kernel(piece_ref, *refs, steps):
    whole_ref, buf, in_sems, out_sems = refs[-4:]
    ring = whole_ref.shape[0]
    reads, writes = [], []
    for k, step in enumerate(steps):
        target = whole_ref.at[ring_place(-step, ring)]
        reads.append(pltpu.make_async_copy(piece_ref.at[:, k], buf.at[k], in_sems.at[k]))
        writes.append(pltpu.make_async_copy(buf.at[k], target, out_sems.at[k]))
    for copy in reads:
        copy.start()
    for read, write in zip(reads, writes):
        read.wait()
        write.start()
    for copy in writes:
        copy.wait()


def place(whole, ring, piece, steps):
    plane, _, *block = piece.shape
    n = len(steps)
    args = (piece,) if whole is None else (piece, whole)
    return pl.pallas_call(
        functools.partial(place_kernel, steps=steps),
        compiler_params=WIDE,
        in_specs=[IN_HBM] * len(args),
        out_specs=IN_HBM,
        out_shape=jax.ShapeDtypeStruct((ring, plane, *block), jnp.float32),
        scratch_shapes=[
            pltpu.VMEM((n, plane, *block), jnp.float32),
            pltpu.SemaphoreType.DMA((n,)),
            pltpu.SemaphoreType.DMA((n,)),
        ],
        input_output_aliases={} if whole is None else {1: 0},
    )(*args)


def place_pair_kernel(*refs, steps):
    n = len(steps)
    block_refs, whole_ref, sems = refs[:n], refs[n + 1], refs[n + 2]
    ring = whole_ref.shape[0]
    part = block_refs[0].shape[0] // PIECES
    copies = []
    for k, step in enumerate(steps):
        for p in range(PIECES):
            source = block_refs[k].at[pl.ds(p * part, part)]
            target = whole_ref.at[ring_place(-step, ring), pl.ds(p * part, part)]
            copies.append(pltpu.make_async_copy(source, target, sems.at[k, p]))
    for copy in copies:
        copy.start()
    for copy in copies:
        copy.wait()


def place_blocks(whole, blocks, steps, near):
    n = len(steps)
    if near:
        blocks = [pltpu.with_memory_space_constraint(block, pltpu.VMEM) for block in blocks]
    return pl.pallas_call(
        functools.partial(place_pair_kernel, steps=steps),
        compiler_params=LIMIT if near else WIDE,
        in_specs=[IN_VMEM] * n + [IN_HBM],
        out_specs=IN_HBM,
        out_shape=jax.ShapeDtypeStruct(whole.shape, jnp.float32),
        scratch_shapes=[pltpu.SemaphoreType.DMA((n, PIECES))],
        input_output_aliases={n: 0},
    )(*blocks, whole)


def shifted(block, ring, step):
    return lax.ppermute(block, "space_0", [(i, (i + step) % ring) for i in range(ring)])


def exchanged(value, axes):
    return lax.all_to_all(value, axes, split_axis=0, concat_axis=0, tiled=True)


def per_device(precip):
    by_row = jnp.transpose(precip, (1, 0, 2))
    stays = pltpu.with_memory_space_constraint(by_row, pltpu.HBM)
    rows, days, lon = by_row.shape
    ring = lax.axis_size("space_0")
    plane = lax.axis_size("space_1") * lax.axis_size("space_2")
    blocks = lax.axis_size("tm")

    def sent(block, step):
        return shifted(block, ring, step)

    raw = [sent(lead_column(stays, ring, RING_FIRST[0]), RING_FIRST[0])]
    cut = cut_columns(stays, ring, RING_FIRST[1:])
    raw += [sent(cut[k - 1], RING_FIRST[k]) for k in (1, 2)]
    theirs = block_totals(stays, blocks)
    theirs = exchanged(theirs, "tm")
    mixed = running_columns(stays, theirs, ring, PLANE_FIRST, plane)
    mixed = exchanged(mixed, PLANE)
    lines = carry_lines(theirs, RING_FIRST, ring)
    lines = [sent(line, step) for line, step in zip(lines, RING_FIRST)]
    late = [sent(mixed[:, k], PLANE_FIRST[k]) for k in range(1, len(PLANE_FIRST))]
    second = running_blocks(raw, lines, plane)
    second = exchanged(second, PLANE)
    whole = place(None, ring, mixed, (0,))
    whole = place_blocks(whole, late[2:], PLANE_FIRST[3:], False)
    whole = place(whole, ring, second, RING_FIRST)
    whole = place_blocks(whole, late[:2], PLANE_FIRST[1:3], True)
    return whole.reshape(ring * plane * rows, lon // (ring * plane), days)


def solution(mesh):
    finer = Mesh(
        mesh.devices.reshape(8, 4, 2, mesh.shape["tm"]), ("space_0", "space_1", "space_2", "tm")
    )
    space = ("space_0", "space_1", "space_2")
    return jax.shard_map(
        per_device,
        mesh=finer,
        in_specs=(P("tm", space, None),),
        out_specs=P(None, space, "tm"),
        check_vma=False,
    )
```

```python
import functools

import jax
import jax.numpy as jnp
from jax import lax
from jax.experimental import pallas as pl
from jax.experimental.pallas import tpu as pltpu
from jax.sharding import Mesh
from jax.sharding import PartitionSpec as P

PLANE = ("space_1", "space_2")
RING_FIRST = (4, -3, 3)
PLANE_FIRST = (0, -1, 1, -2, 2)
PARTS = 3

IN_VMEM = pl.BlockSpec(memory_space=pltpu.VMEM)
IN_HBM = pl.BlockSpec(memory_space=pl.ANY)
LIMIT = pltpu.CompilerParams(vmem_limit_bytes=12 * 2**20)
JOIN = pltpu.CompilerParams(vmem_limit_bytes=65_300_000)
WIDE = pltpu.CompilerParams(vmem_limit_bytes=64_800_000)


def hbm(shape):
    return pltpu.HBM(shape, jnp.float32)


def ring_place(step, ring):
    return lax.rem(lax.axis_index("space_0") + (step + ring), ring)


def carried(theirs_ref, blocks_before, row, lanes):
    carry = None
    for q in range(theirs_ref.shape[0]):
        line = jnp.where(q < blocks_before, theirs_ref[q, pl.ds(row, 1), lanes], 0.0)
        carry = line if carry is None else carry + line
    return carry


def running_kernel(sources, carry_of, out_ref, days_buf, parts_buf, out_buf, in_sems, out_sems):
    n = len(sources)
    rows, days, width = days_buf.shape[1:]
    plane, cell = out_buf.shape[1], out_buf.shape[3]
    reads = [pltpu.make_async_copy(sources[k], days_buf.at[k], in_sems.at[k]) for k in range(n)]
    writes = [
        pltpu.make_async_copy(out_buf.at[k], out_ref.at[:, k], out_sems.at[k]) for k in range(n)
    ]
    for copy in reads:
        copy.start()
    earlier = lax.broadcasted_iota(jnp.int32, (days, days), 0)
    later = lax.broadcasted_iota(jnp.int32, (days, days), 1)
    upto = (earlier <= later).astype(jnp.bfloat16)
    upto = jnp.concatenate([upto] * PARTS, 0)
    first = lax.broadcasted_iota(jnp.int32, (days, width), 0) == 0
    for k in range(n):
        reads[k].wait()
        for r in range(rows):
            x = days_buf[k, r]
            x = jnp.where(first, x + carry_of(k, r), x).T
            for p in range(PARTS):
                part = x.astype(jnp.bfloat16)
                parts_buf[k % 2, r, :, pl.ds(p * days, days)] = part
                x = x - part.astype(jnp.float32)
        for r in range(rows):
            total = jnp.dot(parts_buf[k % 2, r], upto, preferred_element_type=jnp.float32)
            out_buf[k, :, r] = total.reshape(plane, cell, days)
        writes[k].start()
    for copy in writes:
        copy.wait()


def column_kernel(days_ref, theirs_ref, out_ref, *scratch, steps, ring):
    width = days_ref.shape[2] // ring
    lanes = [
        pl.ds(pl.multiple_of(ring_place(s, ring) * width, width), width) for s in steps
    ]
    running_kernel(
        [days_ref.at[:, :, part] for part in lanes],
        lambda k, r: carried(theirs_ref, lax.axis_index("tm"), r, lanes[k]),
        out_ref,
        *scratch,
    )


def cut_kernel(days_ref, *refs, steps, ring):
    n = len(steps)
    out_refs, buf, in_sems, out_sems = refs[:n], refs[n], refs[n + 1], refs[n + 2]
    width = days_ref.shape[2] // ring
    reads, writes = [], []
    for k, step in enumerate(steps):
        lanes = pl.ds(pl.multiple_of(ring_place(step, ring) * width, width), width)
        reads.append(pltpu.make_async_copy(days_ref.at[:, :, lanes], buf.at[k], in_sems.at[k]))
        writes.append(pltpu.make_async_copy(buf.at[k], out_refs[k], out_sems.at[k]))
    for copy in reads:
        copy.start()
    for read, write in zip(reads, writes):
        read.wait()
        write.start()
    for copy in writes:
        copy.wait()


def cut_columns(by_row, ring, steps):
    rows, days, lon = by_row.shape
    n = len(steps)
    shape = (rows, days, lon // ring)
    return pl.pallas_call(
        functools.partial(cut_kernel, steps=steps, ring=ring),
        compiler_params=LIMIT,
        in_specs=[IN_HBM],
        out_specs=[IN_HBM] * n,
        out_shape=[hbm(shape)] * n,
        scratch_shapes=[
            pltpu.VMEM((n, *shape), jnp.float32),
            pltpu.SemaphoreType.DMA((n,)),
            pltpu.SemaphoreType.DMA((n,)),
        ],
    )(by_row)


def lead_kernel(days_ref, out_ref, sem, *, step, ring):
    width = days_ref.shape[2] // ring
    lanes = pl.ds(pl.multiple_of(ring_place(step, ring) * width, width), width)
    copy = pltpu.make_async_copy(days_ref.at[:, :, lanes], out_ref, sem)
    copy.start()
    copy.wait()


def lead_column(by_row, ring, step):
    rows, days, lon = by_row.shape
    return pl.pallas_call(
        functools.partial(lead_kernel, step=step, ring=ring),
        compiler_params=LIMIT,
        in_specs=[IN_HBM],
        out_specs=IN_VMEM,
        out_shape=pltpu.VMEM((rows, days, lon // ring), jnp.float32),
        scratch_shapes=[pltpu.SemaphoreType.DMA],
    )(by_row)


def block_kernel(*refs, n):
    blocks, lines, rest = refs[:n], refs[n : 2 * n], refs[2 * n :]
    out_ref, *scratch = rest[-6:]
    running_kernel(blocks, lambda k, r: lines[k][pl.ds(r, 1)], out_ref, *scratch)


def running_call(body, specs, args, n, rows, days, width, plane, params=LIMIT):
    cell = width // plane
    return pl.pallas_call(
        body,
        compiler_params=params,
        in_specs=specs,
        out_specs=IN_HBM,
        out_shape=hbm((plane, n, rows, cell, days)),
        scratch_shapes=[
            pltpu.VMEM((n, rows, days, width), jnp.float32),
            pltpu.VMEM((2, rows, width, PARTS * days), jnp.bfloat16),
            pltpu.VMEM((n, plane, rows, cell, days), jnp.float32),
            pltpu.SemaphoreType.DMA((n,)),
            pltpu.SemaphoreType.DMA((n,)),
        ],
    )(*args)


def running_columns(by_row, theirs, ring, steps, plane):
    rows, days, lon = by_row.shape
    body = functools.partial(column_kernel, steps=steps, ring=ring)
    specs = [IN_HBM, IN_VMEM]
    args = (by_row, theirs)
    return running_call(body, specs, args, len(steps), rows, days, lon // ring, plane)


def running_blocks(blocks, lines, plane):
    n = len(blocks)
    body = functools.partial(block_kernel, n=n)
    specs = [IN_HBM] * n + [IN_VMEM] * n
    return running_call(body, specs, (*blocks, *lines), n, *blocks[0].shape, plane, JOIN)


def totals_kernel(days_ref, total_ref, days_buf, sems):
    rows, _, lon = days_ref.shape
    cuts = sems.shape[0]
    width = lon // cuts
    copies = [
        pltpu.make_async_copy(
            days_ref.at[:, :, pl.ds(c * width, width)], days_buf.at[:, :, pl.ds(c * width, width)], sems.at[c]
        )
        for c in range(cuts)
    ]
    for copy in copies:
        copy.start()
    for c in range(cuts):
        copies[c].wait()
        for r in range(rows):
            line = jnp.sum(days_buf[r, :, pl.ds(c * width, width)], axis=0, keepdims=True)
            for q in range(total_ref.shape[0]):
                total_ref[q, pl.ds(r, 1), pl.ds(c * width, width)] = line


def block_totals(by_row, copies, cuts=8):
    rows, _, lon = by_row.shape
    return pl.pallas_call(
        totals_kernel,
        compiler_params=LIMIT,
        in_specs=[IN_HBM],
        out_specs=IN_VMEM,
        out_shape=jax.ShapeDtypeStruct((copies, rows, lon), jnp.float32),
        scratch_shapes=[pltpu.VMEM(by_row.shape, jnp.float32), pltpu.SemaphoreType.DMA((cuts,))],
    )(by_row)


def lines_kernel(theirs_ref, *line_refs, steps, ring):
    width = theirs_ref.shape[2] // ring
    for step, line_ref in zip(steps, line_refs):
        lanes = pl.ds(pl.multiple_of(ring_place(step, ring) * width, width), width)
        line_ref[...] = jnp.zeros_like(line_ref)
        for r in range(theirs_ref.shape[1]):
            line_ref[pl.ds(r, 1)] = carried(theirs_ref, lax.axis_index("tm"), r, lanes)


def carry_lines(theirs, steps, ring):
    width = theirs.shape[2] // ring
    return pl.pallas_call(
        functools.partial(lines_kernel, steps=steps, ring=ring),
        compiler_params=LIMIT,
        in_specs=[IN_VMEM],
        out_specs=[IN_VMEM] * len(steps),
        out_shape=[jax.ShapeDtypeStruct((8, width), jnp.float32)] * len(steps),
    )(theirs)


def place_kernel(piece_ref, *refs, steps):
    whole_ref, buf, in_sems, out_sems = refs[-4:]
    ring = whole_ref.shape[0]
    reads, writes = [], []
    for k, step in enumerate(steps):
        target = whole_ref.at[ring_place(-step, ring)]
        reads.append(pltpu.make_async_copy(piece_ref.at[:, k], buf.at[k], in_sems.at[k]))
        writes.append(pltpu.make_async_copy(buf.at[k], target, out_sems.at[k]))
    for copy in reads:
        copy.start()
    for read, write in zip(reads, writes):
        read.wait()
        write.start()
    for copy in writes:
        copy.wait()


def place(whole, ring, piece, steps):
    plane, _, *block = piece.shape
    n = len(steps)
    args = (piece,) if whole is None else (piece, whole)
    return pl.pallas_call(
        functools.partial(place_kernel, steps=steps),
        compiler_params=WIDE,
        in_specs=[IN_HBM] * len(args),
        out_specs=IN_HBM,
        out_shape=jax.ShapeDtypeStruct((ring, plane, *block), jnp.float32),
        scratch_shapes=[
            pltpu.VMEM((n, plane, *block), jnp.float32),
            pltpu.SemaphoreType.DMA((n,)),
            pltpu.SemaphoreType.DMA((n,)),
        ],
        input_output_aliases={} if whole is None else {1: 0},
    )(*args)


def place_pair_kernel(*refs, steps):
    n = len(steps)
    block_refs, whole_ref, sems = refs[:n], refs[n + 1], refs[n + 2]
    ring = whole_ref.shape[0]
    copies = [
        pltpu.make_async_copy(
            block_refs[k], whole_ref.at[ring_place(-step, ring)], sems.at[k]
        )
        for k, step in enumerate(steps)
    ]
    for copy in copies:
        copy.start()
    for copy in copies:
        copy.wait()


def place_blocks(whole, blocks, steps, near):
    n = len(steps)
    if near:
        blocks = [pltpu.with_memory_space_constraint(block, pltpu.VMEM) for block in blocks]
    return pl.pallas_call(
        functools.partial(place_pair_kernel, steps=steps),
        compiler_params=LIMIT if near else WIDE,
        in_specs=[IN_VMEM] * n + [IN_HBM],
        out_specs=IN_HBM,
        out_shape=jax.ShapeDtypeStruct(whole.shape, jnp.float32),
        scratch_shapes=[pltpu.SemaphoreType.DMA((n,))],
        input_output_aliases={n: 0},
    )(*blocks, whole)


def shifted(block, ring, step):
    return lax.ppermute(block, "space_0", [(i, (i + step) % ring) for i in range(ring)])


def exchanged(value, axes):
    return lax.all_to_all(value, axes, split_axis=0, concat_axis=0, tiled=True)


def per_device(precip):
    by_row = jnp.transpose(precip, (1, 0, 2))
    stays = pltpu.with_memory_space_constraint(by_row, pltpu.HBM)
    rows, days, lon = by_row.shape
    ring = lax.axis_size("space_0")
    plane = lax.axis_size("space_1") * lax.axis_size("space_2")
    blocks = lax.axis_size("tm")

    def sent(block, step):
        return shifted(block, ring, step)

    raw = [sent(lead_column(stays, ring, RING_FIRST[0]), RING_FIRST[0])]
    cut = cut_columns(stays, ring, RING_FIRST[1:])
    raw += [sent(cut[k - 1], RING_FIRST[k]) for k in (1, 2)]
    theirs = block_totals(stays, blocks)
    theirs = exchanged(theirs, "tm")
    mixed = running_columns(stays, theirs, ring, PLANE_FIRST, plane)
    mixed = exchanged(mixed, PLANE)
    lines = carry_lines(theirs, RING_FIRST, ring)
    lines = [sent(line, step) for line, step in zip(lines, RING_FIRST)]
    late = [sent(mixed[:, k], PLANE_FIRST[k]) for k in range(1, len(PLANE_FIRST))]
    second = running_blocks(raw, lines, plane)
    second = exchanged(second, PLANE)
    whole = place(None, ring, mixed, (0,))
    whole = place_blocks(whole, late[2:], PLANE_FIRST[3:], False)
    whole = place(whole, ring, second, RING_FIRST)
    whole = place_blocks(whole, late[:2], PLANE_FIRST[1:3], True)
    return whole.reshape(ring * plane * rows, lon // (ring * plane), days)


def solution(mesh):
    finer = Mesh(
        mesh.devices.reshape(8, 4, 2, mesh.shape["tm"]), ("space_0", "space_1", "space_2", "tm")
    )
    space = ("space_0", "space_1", "space_2")
    return jax.shard_map(
        per_device,
        mesh=finer,
        in_specs=(P("tm", space, None),),
        out_specs=P(None, space, "tm"),
        check_vma=False,
    )
```
